32 devices in a mesh: orb: 8 (over z, x), aux: 4 (over y, core).
Axes of the slice: x: 2, y: 2, z: 4, core: 2. Of those that a mesh axis runs over, the one named last changes fastest.
Arguments:
- orbital_factors: bfloat16 [32, 384, 1536], P('orb', None, 'aux'), may hold values from -1 to 1
- metric_factor: bfloat16 [1536, 1536], P(None, 'aux'), may hold values from -0.15625 to 0.15625
- occ_energy: float32 [32], replicated, may hold values from -2 to -0.3
- vir_energy: float32 [384], replicated, may hold values from 0.2 to 3
- pair_list: int32 [48, 2], P('orb'), may hold values from 0 to 31, as said below
Outputs:
- gradient_factors: bfloat16 [32, 384, 1536], P('orb', None, 'aux')
The draws below stay inside these ranges and needn't reach their ends.
Inputs may be any that keep to these rules, and one draw needn't show every extreme that they name: `pair_list`: row r belongs to device r // 6 of orb, where orbital o is owned by device o // 4; its first entry is an orbital of that device; its second is an orbital of the device (r % 6) % 3 - 1 places further along orb, or of the row's own device where that place lies outside orb.
All inputs are finite; a program needn't handle non-finite values.
Results may differ from the reference program's by a relative error of at most 0.0083.
Values may be sent and summed in bfloat16 or wider, within the bound.
No kernel may reach another device: no remote copies, remote signals or barrier semaphores. Data moves between devices by JAX's collectives and lax.ppermute only.
A program may use at most 64 MiB of HBM per device.

```python
import jax
import jax.numpy as jnp
from jax import lax

V = 384
NAUX = 1536
OCC_DEV = 4
PAIRS_DEV = 6
NOCC = 32


def draw_pair_list(key, part):
    owners = NOCC // OCC_DEV
    row_total = owners * PAIRS_DEV
    device = jnp.arange(row_total, dtype=jnp.int32) // PAIRS_DEV
    slot_ids = jnp.arange(row_total, dtype=jnp.int32) % PAIRS_DEV
    partner = jnp.clip(device + slot_ids % 3 - 1, 0, owners - 1)
    first_key, second_key = jax.random.split(jax.random.fold_in(key, 17))
    left_index = device * OCC_DEV + jax.random.randint(first_key, (row_total,), 0, OCC_DEV, dtype=jnp.int32)
    right_index = partner * OCC_DEV + jax.random.randint(second_key, (row_total,), 0, OCC_DEV, dtype=jnp.int32)
    return jnp.stack([left_index, right_index], axis=1).astype(jnp.int32)


def shard_levels(own_key, dims, cuts, least, high):
    gain = 1.0
    for dim, blocks in cuts:
        heights = jax.random.uniform(jax.random.fold_in(jax.random.fold_in(own_key, 6), dim), (blocks,), jnp.float32, least / len(cuts), high / len(cuts))
        gain = gain * jnp.repeat(jnp.exp(heights), dims[dim] // blocks).reshape((-1,) + (1,) * (len(dims) - 1 - dim))
    return gain


def scatter_about(own_key, dims, spread, most, cuts=(), kind=jnp.bfloat16):
    loudness = shard_levels(own_key, dims, cuts, -0.22, 0.18) if cuts else 1.0
    array = jax.random.normal(own_key, dims, jnp.float32) * spread * loudness
    return jnp.minimum(jnp.maximum(array, -most), most).astype(kind)


def setup_inputs(seed: int = 0) -> dict:
    key_of = jax.random.split(jax.random.key(seed), 6)
    orbital_factors = scatter_about(key_of[0], (NOCC, V, NAUX), 0.16, 1.0, ((0, 8), (2, 4)))
    metric_factor = scatter_about(key_of[1], (NAUX, NAUX), NAUX ** -0.5, 0.15625, ((1, 4),))
    occ_energy = jnp.clip(jax.random.uniform(key_of[2], (NOCC,), jnp.float32, -2.0, -0.3), -2.0, -0.3)
    vir_energy = jnp.clip(jax.random.uniform(key_of[3], (V,), jnp.float32, 0.2, 3.0), 0.2, 3.0)
    pair_list = draw_pair_list(jax.random.fold_in(key_of[5], 71), 0)
    return dict(orbital_factors=orbital_factors, metric_factor=metric_factor, occ_energy=occ_energy, vir_energy=vir_energy, pair_list=pair_list)


def reference(orbital_factors, metric_factor, occ_energy, vir_energy, pair_list):
    def add_pair(density_sum, pair_row):
        left_index = pair_row[0]
        right_index = pair_row[1]
        left_block = lax.dynamic_index_in_dim(orbital_factors, left_index, 0, keepdims=False)
        right_block = lax.dynamic_index_in_dim(orbital_factors, right_index, 0, keepdims=False)
        integrals = jnp.dot(left_block, right_block.T, preferred_element_type=jnp.float32)
        denominator = (occ_energy[left_index] + occ_energy[right_index]) - vir_energy[:, None] - vir_energy[None, :]
        amplitudes = (integrals / denominator).astype(jnp.bfloat16)
        left_term = jnp.dot(amplitudes, right_block, preferred_element_type=jnp.float32)
        right_term = jnp.dot(amplitudes.T, left_block, preferred_element_type=jnp.float32)
        density_sum = density_sum.at[left_index].add(left_term)
        density_sum = density_sum.at[right_index].add(right_term)
        return density_sum, None

    start_sum = jnp.zeros(orbital_factors.shape, jnp.float32)
    density_sum, unused = lax.scan(add_pair, start_sum, pair_list)
    density = density_sum.astype(jnp.bfloat16)
    flat = density.reshape(-1, NAUX)
    result = jnp.dot(flat, metric_factor, preferred_element_type=jnp.float32)
    return result.astype(jnp.bfloat16).reshape(NOCC, V, NAUX)
```

```python
import functools

import jax
import jax.numpy as jnp
from jax import lax
from jax.experimental import pallas as pl
from jax.experimental.pallas import tpu as pltpu
from jax.sharding import PartitionSpec as P


F32 = jnp.float32
BF16 = jnp.bfloat16
VM = pl.BlockSpec(memory_space=pltpu.VMEM)
SM = pl.BlockSpec(memory_space=pltpu.SMEM)
PHASES = (0, 1)


def struct(shape, dtype):
    return jax.ShapeDtypeStruct(shape, dtype)


def call(body, outs, in_specs, name, flops, args, scratch=(), limit=16):
    with jax.named_scope(name):
        moved = sum(a.size * a.dtype.itemsize for a in args)
        return pl.pallas_call(
            body,
            out_shape=outs,
            in_specs=in_specs,
            out_specs=jax.tree.map(lambda _: VM, outs),
            scratch_shapes=scratch,
            name=name,
            compiler_params=pltpu.CompilerParams(vmem_limit_bytes=limit << 20),
            cost_estimate=pl.CostEstimate(flops=int(flops), bytes_accessed=int(moved), transcendentals=0),
        )(*args)


def mate(place, phase):
    return ((place + phase) ^ 1) - phase


def meeting(phase):
    g = lax.axis_index("orb")
    right = 1 - jnp.bitwise_and(g + phase, 1)
    other = g + 2 * right - 1
    return right, jnp.logical_or(other < 0, other >= lax.axis_size("orb"))


def phase_pair(phase, s, own, came):
    right, alone = meeting(phase)
    i, j = [jnp.where(alone, own[3 * s + 2 * right, c], came[3 * s + 2 * (1 - right), c]) for c in (0, 1)]
    return i, j, alone


def nt_dot(a, b):
    return lax.dot_general(a, b, (((1,), (1,)), ((), ())), preferred_element_type=F32)


def tn_dot(a, b):
    return lax.dot_general(a, b, (((0,), (0,)), ((), ())), preferred_element_type=F32)


def nn_dot(a, b):
    return lax.dot_general(a, b, (((1,), (0,)), ((), ())), preferred_element_type=F32)


def halves(half):
    mine = jnp.bitwise_and(lax.axis_index("aux"), 1)
    return pl.multiple_of(mine * half, half), pl.multiple_of((1 - mine) * half, half)


def pick_body(count, own, factors, *outs):
    owned = factors.shape[0]
    for phase in PHASES:
        right, _ = meeting(phase)
        for s in range(count):
            outs[phase][s] = factors[lax.rem(own[3 * s + 2 * right, 0], owned)]


def integrals_body(phase, own, came, factors, arrived, keep, send):
    count, half, _ = keep.shape
    owned = factors.shape[0]
    mine, other = halves(half)
    for s in range(count):
        i, j, alone = phase_pair(phase, s, own, came)
        at = lax.rem(i, owned)
        second = factors[lax.rem(j, owned)]
        rows = jnp.where(alone, factors[at, pl.ds(other, half), :], arrived[s, pl.ds(other, half), :])
        send[s] = nt_dot(rows, second).astype(BF16)
        rows = jnp.where(alone, factors[at, pl.ds(mine, half), :], arrived[s, pl.ds(mine, half), :])
        keep[s] = nt_dot(rows, second)


def add_body(held, came, total, send):
    total[...] = held[...] + came[...].astype(F32)
    send[...] = total[...].astype(BF16)


def amplitudes_body(phase, own, other_list, occ, column, row, held, came, out):
    count, half, _ = held.shape
    mine, _ = halves(half)
    for s in range(count):
        i, j, _ = phase_pair(phase, s, own, other_list)
        denominator = (occ[i] + occ[j]) - column[pl.ds(mine, half), :] - row[...]
        out[s] = ((held[s] + came[s].astype(F32)) / denominator).astype(BF16)


def terms_body(phase, own, other_list, factors, arrived, moved, amps, came, density, back, whole):
    count, half, _ = amps.shape
    owned = factors.shape[0]
    mine, other = halves(half)
    for s in range(count):
        i, j, alone = phase_pair(phase, s, own, other_list)
        whole[s, pl.ds(mine, half), :] = amps[s]
        whole[s, pl.ds(other, half), :] = came[s]
        back[s] = nn_dot(whole[s], moved[lax.rem(j, owned)]).astype(BF16)
        first = jnp.where(alone, factors[lax.rem(i, owned)], arrived[s])
        density[s] = tn_dot(whole[s], first).astype(BF16)


def through_metric(blocks, metric, at):
    me = lax.axis_index("aux")
    width = blocks[0].shape[-1]
    total = None
    for offset, block in enumerate(blocks):
        start = pl.multiple_of(jnp.bitwise_xor(me, offset) * width, width)
        term = nn_dot(block[at], metric[pl.ds(start, width), :])
        total = term if total is None else total + term
    return total


def moved_body(metric, *refs):
    blocks, out = refs[:-1], refs[-1]
    for o in range(out.shape[0]):
        out[o] = through_metric(blocks, metric, o).astype(BF16)


def own_amplitudes_body(own, occ, column, row, *refs):
    blocks, out = refs[:-1], refs[-1]
    count, rows, _ = out.shape
    owned = blocks[0].shape[0]
    start = pl.multiple_of(lax.shift_right_logical(lax.axis_index("aux"), 1) * rows, rows)
    for s in range(count):
        i, j = own[3 * s + 1, 0], own[3 * s + 1, 1]
        total = None
        for block in blocks:
            term = nt_dot(block[lax.rem(i, owned), pl.ds(start, rows), :], block[lax.rem(j, owned)])
            total = term if total is None else total + term
        denominator = (occ[i] + occ[j]) - column[pl.ds(start, rows), :] - row[...]
        out[s] = (total / denominator).astype(BF16)


def own_terms_body(own, moved, *refs):
    parts, out, whole = refs[:-2], refs[-2], refs[-1]
    owned = moved.shape[0]
    count, rows, _ = parts[0].shape
    me = lax.shift_right_logical(lax.axis_index("aux"), 1)
    out[...] = jnp.zeros_like(out)
    for s in range(count):
        for offset, part in enumerate(parts):
            start = pl.multiple_of(jnp.bitwise_xor(me, offset) * rows, rows)
            whole[s, pl.ds(start, rows), :] = part[s]
        i, j = lax.rem(own[3 * s + 1, 0], owned), lax.rem(own[3 * s + 1, 1], owned)
        out[i] += nn_dot(whole[s], moved[j])
        out[j] += tn_dot(whole[s], moved[i])


def finish_body(phase, size, own, other_list, held, metric, *refs):
    blocks = refs[:size]
    back, came, out = refs[size : size + 3]
    total = refs[size + 3] if len(refs) > size + 3 else out
    owned = held.shape[0]
    count = back.shape[0]
    total[...] = held[...]
    right, _ = meeting(phase)
    for s in range(count):
        _, j, alone = phase_pair(phase, s, own, other_list)
        total[lax.rem(j, owned)] += through_metric(blocks, metric, s)
        at = lax.rem(own[3 * s + 2 * right, 0], owned)
        total[at] += jnp.where(alone, back[s], came[s]).astype(F32)
    if total is not out:
        out[...] = total[...].astype(BF16)


def flip(value, bit, name):
    with jax.named_scope(name):
        size = lax.axis_size("aux")
        return lax.ppermute(value, "aux", [(k, k ^ (1 << bit)) for k in range(size)])


def meet(value, phase, name):
    with jax.named_scope(name):
        size = lax.axis_size("orb")
        swaps = [(k, mate(k, phase)) for k in range(size) if 0 <= mate(k, phase) < size]
        return lax.ppermute(value, "orb", swaps)


def gathered(block, bits, name):
    blocks = {0: block}
    for bit in reversed(range(bits)):
        blocks.update({o ^ (1 << bit): flip(b, bit, f"{name}{o}_{bit}") for o, b in list(blocks.items())})
    return [blocks[o] for o in range(1 << bits)]


def local(orbital_factors, metric_factor, occ_energy, vir_energy, pair_list):
    owned, virtuals, width = orbital_factors.shape
    columns = metric_factor.shape[1]
    size = lax.axis_size("aux")
    bits = size.bit_length() - 1
    assert size == 1 << bits and bits >= 2
    count = pair_list.shape[0] // 3
    half = virtuals // 2
    parts = size // 2
    cube = 2 * virtuals * virtuals * width
    column = vir_energy[:, None]
    row = vir_energy[None, :]
    wide, narrow = (struct((count, half, virtuals), t) for t in (F32, BF16))

    sends = call(
        functools.partial(pick_body, count),
        [struct((count, virtuals, width), BF16)] * 2,
        [SM, VM],
        "pick",
        cube // 8,
        (pair_list, orbital_factors),
    )
    arrived = [meet(sends[x], x, f"halo{x}") for x in PHASES]
    lists = [meet(pair_list, x, f"list{x}") for x in PHASES]
    blocks = gathered(orbital_factors, bits, "factors")
    moved = call(
        moved_body,
        struct((owned, virtuals, columns), BF16),
        [VM] * (1 + size),
        "moved",
        cube * owned * size,
        (metric_factor, *blocks),
    )

    amps = []
    for x in PHASES:
        keep, send = call(
            functools.partial(integrals_body, x),
            [wide, narrow],
            [SM] * 2 + [VM] * 2,
            f"integrals{x}",
            count * cube,
            (pair_list, lists[x], orbital_factors, arrived[x]),
        )
        for bit in range(bits - 1):
            keep, send = call(
                add_body, [wide, narrow], [VM] * 2, f"add{x}", cube // 8, (keep, flip(send, bit, f"sum{x}_{bit}"))
            )
        amps.append(
            call(
                functools.partial(amplitudes_body, x),
                narrow,
                [SM] * 3 + [VM] * 4,
                f"amplitudes{x}",
                cube // 8,
                (pair_list, lists[x], occ_energy, column, row, keep, flip(send, bits - 1, f"sum{x}_{bits - 1}")),
            )
        )

    own_amps = call(
        own_amplitudes_body,
        struct((count, virtuals // parts, virtuals), BF16),
        [SM] * 2 + [VM] * (2 + size),
        "own_amplitudes",
        cube * count * size // parts,
        (pair_list, occ_energy, column, row, *blocks),
    )
    own_parts = {0: own_amps}
    for bit in range(1, bits):
        own_parts.update(
            {o ^ (1 << (bit - 1)): flip(b, bit, f"own{o}_{bit}") for o, b in list(own_parts.items())}
        )
    held = call(
        own_terms_body,
        struct((owned, virtuals, columns), F32),
        [SM] + [VM] * (1 + parts),
        "own_terms",
        2 * count * cube,
        (pair_list, moved, *[own_parts[o] for o in range(parts)]),
        [pltpu.VMEM((count, virtuals, virtuals), BF16)],
    )
    for x in PHASES:
        density, back = call(
            functools.partial(terms_body, x),
            [struct((count, virtuals, width), BF16), struct((count, virtuals, columns), BF16)],
            [SM] * 2 + [VM] * 5,
            f"terms{x}",
            2 * count * cube,
            (pair_list, lists[x], orbital_factors, arrived[x], moved, amps[x], flip(amps[x], 0, f"join{x}")),
            [pltpu.VMEM((count, virtuals, virtuals), BF16)],
        )
        came = meet(back, x, f"back{x}")
        density_blocks = gathered(density, bits, f"density{x}_")
        final = x == PHASES[-1]
        held = call(
            functools.partial(finish_body, x, size),
            struct((owned, virtuals, columns), BF16 if final else F32),
            [SM] * 2 + [VM] * (4 + size),
            f"finish{x}",
            count * size * cube,
            (pair_list, lists[x], held, metric_factor, *density_blocks, back, came),
            [pltpu.VMEM((owned, virtuals, columns), F32)] if final else [],
        )
    return held


def solution(mesh):
    placed = (P("orb", None, "aux"), P(None, "aux"), P(), P(), P("orb", None))
    return jax.shard_map(
        local, mesh=mesh, in_specs=placed, out_specs=P("orb", None, "aux"), check_vma=False
    )
```

```python
import functools

import jax
import jax.numpy as jnp
from jax import lax
from jax.experimental import pallas as pl
from jax.experimental.pallas import tpu as pltpu
from jax.sharding import PartitionSpec as P


F32 = jnp.float32
BF16 = jnp.bfloat16
VM = pl.BlockSpec(memory_space=pltpu.VMEM)
SM = pl.BlockSpec(memory_space=pltpu.SMEM)
PHASES = (0, 1)


def struct(shape, dtype):
    return jax.ShapeDtypeStruct(shape, dtype)


def call(body, outs, in_specs, flops, args, scratch=(), limit=16, alias=None, out_specs=None):
    moved = sum(a.size * a.dtype.itemsize for a in args)
    done = pl.pallas_call(
        body,
        out_shape=outs,
        in_specs=in_specs,
        out_specs=out_specs or jax.tree.map(lambda _: VM, outs),
        scratch_shapes=scratch,
        input_output_aliases=alias or {},
        compiler_params=pltpu.CompilerParams(vmem_limit_bytes=limit << 20),
        cost_estimate=pl.CostEstimate(flops=int(flops), bytes_accessed=int(moved), transcendentals=0),
    )(*args)
    return list(done) if isinstance(done, tuple) else done


def mate(place, phase):
    return ((place + 1 - phase) ^ 1) - 1 + phase


def meeting(phase):
    g = lax.axis_index("orb")
    right = jnp.bitwise_and(g + phase, 1)
    other = g + 2 * right - 1
    return right, jnp.logical_or(other < 0, other >= lax.axis_size("orb"))


def phase_pair(phase, s, own, came):
    right, alone = meeting(phase)
    i, j = [jnp.where(alone, own[c, 3 * s + 2 * right], came[c, 3 * s + 2 * (1 - right)]) for c in (0, 1)]
    return i, j, alone


def nt_dot(a, b):
    return lax.dot_general(a, b, (((1,), (1,)), ((), ())), preferred_element_type=F32)


def tn_dot(a, b):
    return lax.dot_general(a, b, (((0,), (0,)), ((), ())), preferred_element_type=F32)


def nn_dot(a, b):
    return lax.dot_general(a, b, (((1,), (0,)), ((), ())), preferred_element_type=F32)


def halves(half):
    mine = jnp.bitwise_and(lax.axis_index("aux"), 1)
    return pl.multiple_of(mine * half, half), pl.multiple_of((1 - mine) * half, half)


def pick_body(count, own, factors, *refs):
    outs, sems = refs[:-1], refs[-1]
    owned = factors.shape[0]
    copies = []
    for phase in PHASES:
        right, _ = meeting(phase)
        for s in range(count):
            at = lax.rem(own[0, 3 * s + 2 * right], owned)
            copies.append(pltpu.make_async_copy(factors.at[at], outs[phase].at[s], sems.at[phase, s]))
            copies[-1].start()
    for copy in copies:
        copy.wait()


def integrals_body(phase, own, came, factors, arrived, keep, send, source, early):
    count, half, _ = keep.shape
    owned = factors.shape[0]
    mine, other = halves(half)
    for s in range(count):
        i, j, alone = phase_pair(phase, s, own, came)
        second = factors[lax.rem(j, owned)]
        first = early if s == count - 1 else source.at[s]
        first[...] = jnp.where(alone, factors[lax.rem(i, owned)], arrived[s])
        send[s] = nt_dot(first[pl.ds(other, half), :], second).astype(BF16)
        keep[s] = nt_dot(first[pl.ds(mine, half), :], second)


def chosen_integrals_body(seconds, source, keep, send):
    count, half, _ = keep.shape
    mine, other = halves(half)
    for s in range(count):
        send[s] = nt_dot(source[s, pl.ds(other, half), :], seconds[s]).astype(BF16)
        keep[s] = nt_dot(source[s, pl.ds(mine, half), :], seconds[s])


def add_body(held, came, total, send):
    total[...] = held[...] + came[...].astype(F32)
    send[...] = total[...].astype(BF16)


def facts_body(own, *refs):
    lists, (occ, column, row, factors), outs = refs[:2], refs[2:6], refs[6:8]
    seconds, alone_first = refs[8], refs[9:]
    count, half, _ = outs[0].shape
    owned = factors.shape[0]
    mine, _ = halves(half)
    for s in range(count):
        for phase in PHASES:
            i, j, alone = phase_pair(phase, s, own, lists[phase])
            outs[phase][s] = (occ[i] + occ[j]) - column[pl.ds(mine, half), :] - row[...]
        seconds[s] = factors[lax.rem(j, owned)]
        if alone_first:
            first = factors[lax.rem(i, owned)]
            alone_first[0][s] = jnp.where(alone, first, jnp.zeros_like(first))


def choose_body(phase, own, other_list, moved, out):
    for s in range(out.shape[0]):
        _, j, _ = phase_pair(phase, s, own, other_list)
        out[s] = moved[lax.rem(j, moved.shape[0])]


def amplitudes_body(denominators, held, came, out):
    out[...] = ((held[...] + came[...].astype(F32)) / denominators[...]).astype(BF16)


def terms_body(chosen, amps, came, back, whole):
    count, half, _ = amps.shape
    mine, other = halves(half)
    for s in range(count):
        whole[s, pl.ds(mine, half), :] = amps[s]
        whole[s, pl.ds(other, half), :] = came[s]
        back[s] = nn_dot(whole[s], chosen[s]).astype(BF16)


def density_body(source, whole, density):
    for s in range(density.shape[0]):
        density[s] = tn_dot(whole[s], source[s]).astype(BF16)


def metric_rows(metric, offset, width):
    start = jnp.bitwise_xor(lax.axis_index("aux"), offset) * width
    return metric[pl.ds(pl.multiple_of(start, width), width), :]


def moved_body(offsets, first, metric, *refs):
    out = refs[-1]
    blocks = refs[-1 - len(offsets) : -1]
    for o in range(out.shape[0]):
        total = None if first else refs[0][o]
        for offset, block in zip(offsets, blocks):
            term = nn_dot(block[o], metric_rows(metric, offset, block.shape[-1]))
            total = term if total is None else total + term
        out[o] = total.astype(out.dtype)


def moved_last_body(offset, phase, s, own, other_list, metric, held, block, out, picked, chosen):
    moved_body([offset], False, metric, held, block, out)
    right, _ = meeting(phase)
    picked[...] = out[lax.rem(own[0, 3 * s + 2 * right], out.shape[0])]
    choose_body(0, own, other_list, out, chosen)


def own_amplitudes_body(phase, own, other_list, occ, column, row, moved, *refs):
    blocks, out, chosen = refs[:-2], refs[-2], refs[-1]
    choose_body(phase, own, other_list, moved, chosen)
    count, half, _ = out.shape
    owned = blocks[0].shape[0]
    mine, _ = halves(half)
    for s in range(count):
        i, j = own[0, 3 * s + 1], own[1, 3 * s + 1]
        total = None
        for block in blocks:
            term = nt_dot(block[lax.rem(i, owned), pl.ds(mine, half), :], block[lax.rem(j, owned)])
            total = term if total is None else total + term
        denominator = (occ[i] + occ[j]) - column[pl.ds(mine, half), :] - row[...]
        out[s] = (total / denominator).astype(BF16)


def own_terms_body(own, moved, amps, came, out, whole):
    owned = moved.shape[0]
    count, half, _ = amps.shape
    mine, other = halves(half)
    out[...] = jnp.zeros_like(out)
    for s in range(count):
        whole[s, pl.ds(mine, half), :] = amps[s]
        whole[s, pl.ds(other, half), :] = came[s]
        i, j = lax.rem(own[0, 3 * s + 1], owned), lax.rem(own[1, 3 * s + 1], owned)
        out[i] += nn_dot(whole[s], moved[j])
        out[j] += tn_dot(whole[s], moved[i])


def last_pairs_body(early_at, late_at, own, early_list, late_list, held, moved, *refs):
    early_amps, late_amps, traded, metric = refs[:4]
    blocks, out = refs[4:-1], refs[-1]
    owned = moved.shape[0]
    total = None
    for offset, block in enumerate(blocks):
        term = nn_dot(block[...], metric_rows(metric, offset, block.shape[-1]))
        total = term if total is None else total + term
    _, j, _ = phase_pair(*early_at, own, early_list)
    out[lax.rem(j, owned)] += tn_dot(early_amps[early_at[1]], total.astype(BF16))
    i, j, alone = phase_pair(*late_at, own, late_list)
    first = jnp.where(alone, moved[lax.rem(i, owned)], traded[...])
    out[lax.rem(j, owned)] += tn_dot(late_amps[late_at[1]], first)


def result_body(plan, own, lists, held, metric, *refs):
    total = refs[-1]
    owned = held.shape[0]
    for phase, offsets, with_back in plan:
        blocks, refs = refs[: len(offsets)], refs[len(offsets) :]
        for s in range(blocks[0].shape[0]):
            _, j, _ = phase_pair(phase, s, own, lists[phase])
            term = None
            for offset, block in zip(offsets, blocks):
                part = nn_dot(block[s], metric_rows(metric, offset, block.shape[-1]))
                term = part if term is None else term + part
            total[lax.rem(j, owned)] += term
        if with_back:
            (back, came), refs = refs[:2], refs[2:]
            right, alone = meeting(phase)
            for s in range(back.shape[0]):
                at = lax.rem(own[0, 3 * s + 2 * right], owned)
                total[at] += jnp.where(alone, back[s], came[s]).astype(F32)


def result0_body(plan, own, list0, list1, held, metric, *refs):
    result_body(plan, own, (list0, list1), held, metric, *refs)


def result1_body(plan, own, list1, held, metric, *refs):
    *refs, back, weights, total = refs
    result_body(plan, own, (None, list1), held, metric, *refs, total)
    owned = held.shape[0]
    right, alone = meeting(plan[0][0])
    for s in range(back.shape[0]):
        at = lax.rem(own[0, 3 * s + 2 * right], owned)
        for o in range(owned):
            hit = jnp.where(jnp.logical_and(at == o, jnp.logical_not(alone)), 1.0, 0.0).astype(F32)
            weights[o * back.shape[0] + s] = jnp.full(weights.shape[1:], hit, F32)

        @pl.when(alone)
        def _():
            total[at] += back[s].astype(F32)


def last_body(total, weights, came, out, staged, sems):
    owned = total.shape[0]
    count = came.shape[0]
    copies = [pltpu.make_async_copy(staged.at[o], out.at[o], sems.at[o]) for o in range(owned)]
    for o, copy in enumerate(copies):
        value = total[o]
        for s in range(count):
            value = value + weights[o * count + s, 0:1, 0:1] * came[s].astype(F32)
        staged[o] = value.astype(BF16)
        copy.start()
    for copy in copies:
        copy.wait()


def flip(value, bit):
    size = lax.axis_size("aux")
    return lax.ppermute(value, "aux", [(k, k ^ (1 << bit)) for k in range(size)])


def meet(value, phase):
    size = lax.axis_size("orb")
    swaps = [(k, mate(k, phase)) for k in range(size) if 0 <= mate(k, phase) < size]
    return lax.ppermute(value, "orb", swaps)


def gathered(block, bits):
    blocks = {0: block}
    for bit in reversed(range(bits)):
        blocks.update({o ^ (1 << bit): flip(b, bit) for o, b in list(blocks.items())})
    return [blocks[o] for o in range(1 << bits)]


def local(orbital_factors, metric_factor, occ_energy, vir_energy, pair_list):
    owned, virtuals, width = orbital_factors.shape
    columns = metric_factor.shape[1]
    size = lax.axis_size("aux")
    bits = size.bit_length() - 1
    assert size == 1 << bits and bits >= 2
    count = pair_list.shape[0] // 3
    pair_list = pair_list.T
    half = virtuals // 2
    cube = 2 * virtuals * virtuals * width
    column = vir_energy[:, None]
    row = vir_energy[None, :]
    wide, narrow = (struct((count, half, virtuals), t) for t in (F32, BF16))

    sends = call(
        functools.partial(pick_body, count),
        [struct((count, virtuals, width), BF16)] * 2,
        [SM, pl.BlockSpec(memory_space=pltpu.HBM)],
        cube // 8,
        (pair_list, orbital_factors),
        [pltpu.SemaphoreType.DMA((2, count))],
    )
    arrived = [meet(sends[x], x) for x in PHASES]
    lists = [meet(pair_list, x) for x in PHASES]
    blocks = gathered(orbital_factors, bits)
    shape = (owned, virtuals, columns)
    wave = cube * owned
    low = [o for o in range(size) if o < 2]
    moved = call(
        functools.partial(moved_body, low, True),
        struct(shape, F32),
        [VM] * 3,
        2 * wave,
        (metric_factor, *[blocks[o] for o in low]),
    )
    for o in range(2, size - 1):
        moved = call(
            functools.partial(moved_body, [o], False),
            struct(shape, F32),
            [VM] * 3,
            wave,
            (metric_factor, moved, blocks[o]),
            alias={1: 0},
        )
    direct = count - 1
    some = struct((count, virtuals, columns), BF16)
    moved, picked, chosen = call(
        functools.partial(moved_last_body, size - 1, PHASES[-1], direct),
        [struct(shape, BF16), struct((virtuals, columns), BF16), some],
        [SM] * 2 + [VM] * 3,
        wave,
        (pair_list, lists[0], metric_factor, moved, blocks[size - 1]),
    )
    traded = meet(picked, PHASES[-1])

    late, last = PHASES[-1], count - 1
    some = struct((count, virtuals, width), BF16)
    rest = struct((last, virtuals, width), BF16)
    lonely = lax.axis_size("orb") % 2 == 1
    keep0, send0, source0, early = call(
        functools.partial(integrals_body, 0),
        [wide, narrow, rest, struct((virtuals, width), BF16)],
        [SM] * 2 + [VM] * 2,
        count * cube,
        (pair_list, lists[0], orbital_factors, arrived[0]),
    )
    *denominators, seconds, alone_first = call(
        facts_body,
        [wide, wide, some] + [some] * lonely,
        [SM] * 4 + [VM] * 3,
        cube // 8,
        (pair_list, *lists, occ_energy, column, row, orbital_factors),
    ) + [None] * (not lonely)
    source1 = arrived[1] + alone_first if lonely else arrived[1]
    keep1, send1 = call(chosen_integrals_body, [wide, narrow], [VM] * 2, count * cube, (seconds, source1))
    sums = [(keep0, send0), (keep1, send1)]
    sources = [source0, source1]
    early_blocks = gathered(early, bits)

    wholes, gathers = [], []
    for x in PHASES:
        keep, send = sums[x]
        for bit in range(bits - 1):
            keep, send = call(add_body, [wide, narrow], [VM] * 2, cube // 8, (keep, flip(send, bit)))
        amps = call(amplitudes_body, narrow, [VM] * 3, cube // 8, (denominators[x], keep, flip(send, bits - 1)))
        if x == late:
            own_amps, chosen = call(
                functools.partial(own_amplitudes_body, x),
                [narrow, struct((count, virtuals, columns), BF16)],
                [SM] * 3 + [VM] * (3 + size),
                cube * count * size // 2,
                (pair_list, lists[x], occ_energy, column, row, moved, *blocks),
            )
        back, whole = call(
            terms_body,
            [struct((count, virtuals, columns), BF16), struct((count, virtuals, virtuals), BF16)],
            [VM] * 3,
            count * cube,
            (chosen, amps, flip(amps, 0)),
        )
        density = call(density_body, rest, [VM] * 2, last * cube, (sources[x], whole))
        wholes.append(whole)
        gathers.append((gathered(density, bits), back, meet(back, x)))

    held = call(
        own_terms_body,
        struct(shape, F32),
        [SM] + [VM] * 3,
        2 * count * cube,
        (pair_list, moved, own_amps, flip(own_amps, 0)),
        [pltpu.VMEM((count, virtuals, virtuals), BF16)],
    )
    held = call(
        functools.partial(last_pairs_body, (0, last), (late, direct)),
        struct(shape, F32),
        [SM] * 3 + [VM] * (6 + size),
        cube,
        (pair_list, *lists, held, moved, *wholes, traded, metric_factor, *early_blocks),
        alias={3: 0},
    )
    (blocks0, back0, came0), (blocks1, back1, came1) = gathers
    held = call(
        functools.partial(result0_body, [(0, range(size), True), (1, low, False)]),
        struct(shape, F32),
        [SM] * 3 + [VM] * (4 + size + len(low)),
        (size + 2) * last * cube,
        (pair_list, *lists, held, metric_factor, *blocks0, back0, came0, *[blocks1[o] for o in low]),
        alias={3: 0},
    )
    high = range(2, size)
    weights, held = call(
        functools.partial(result1_body, [(1, high, False)]),
        [struct((owned * count, 8, 128), F32), struct(shape, F32)],
        [SM] * 2 + [VM] * (3 + len(high)),
        last * len(high) * cube,
        (pair_list, lists[1], held, metric_factor, *[blocks1[o] for o in high], back1),
        alias={2: 1},
    )
    return call(
        last_body,
        struct(shape, BF16),
        [VM] * 3,
        cube // 8,
        (held, weights, came1),
        [pltpu.VMEM(shape, BF16), pltpu.SemaphoreType.DMA((owned,))],
        out_specs=pl.BlockSpec(memory_space=pltpu.HBM),
    )


def solution(mesh):
    placed = (P("orb", None, "aux"), P(None, "aux"), P(), P(), P("orb", None))
    return jax.shard_map(local, mesh=mesh, in_specs=placed, out_specs=P("orb", None, "aux"), check_vma=False)
```

```python
import functools

import jax
import jax.numpy as jnp
from jax import lax
from jax.experimental import pallas as pl
from jax.experimental.pallas import tpu as pltpu
from jax.sharding import PartitionSpec as P


F32 = jnp.float32
BF16 = jnp.bfloat16
VM = pl.BlockSpec(memory_space=pltpu.VMEM)
SM = pl.BlockSpec(memory_space=pltpu.SMEM)
PHASES = (0, 1)


def struct(shape, dtype):
    return jax.ShapeDtypeStruct(shape, dtype)


def call(body, outs, in_specs, flops, args, scratch=(), limit=16, alias=None, out_specs=None):
    moved = sum(a.size * a.dtype.itemsize for a in args)
    done = pl.pallas_call(
        body,
        out_shape=outs,
        in_specs=in_specs,
        out_specs=out_specs or jax.tree.map(lambda _: VM, outs),
        scratch_shapes=scratch,
        input_output_aliases=alias or {},
        compiler_params=pltpu.CompilerParams(vmem_limit_bytes=limit << 20),
        cost_estimate=pl.CostEstimate(flops=int(flops), bytes_accessed=int(moved), transcendentals=0),
    )(*args)
    return list(done) if isinstance(done, tuple) else done


def mate(place, phase):
    return ((place + 1 - phase) ^ 1) - 1 + phase


def meeting(phase):
    g = lax.axis_index("orb")
    right = jnp.bitwise_and(g + phase, 1)
    other = g + 2 * right - 1
    return right, jnp.logical_or(other < 0, other >= lax.axis_size("orb"))


def phase_pair(phase, s, own, came):
    right, alone = meeting(phase)
    i, j = [jnp.where(alone, own[c, 3 * s + 2 * right], came[c, 3 * s + 2 * (1 - right)]) for c in (0, 1)]
    return i, j, alone


def nt_dot(a, b):
    return lax.dot_general(a, b, (((1,), (1,)), ((), ())), preferred_element_type=F32)


def tn_dot(a, b):
    return lax.dot_general(a, b, (((0,), (0,)), ((), ())), preferred_element_type=F32)


def nn_dot(a, b):
    return lax.dot_general(a, b, (((1,), (0,)), ((), ())), preferred_element_type=F32)


def halves(half):
    mine = jnp.bitwise_and(lax.axis_index("aux"), 1)
    return pl.multiple_of(mine * half, half), pl.multiple_of((1 - mine) * half, half)


def pick_body(count, own, factors, *refs):
    outs, sems = refs[:-1], refs[-1]
    owned = factors.shape[0]
    copies = []
    for phase in PHASES:
        right, _ = meeting(phase)
        for s in range(count):
            at = lax.rem(own[0, 3 * s + 2 * right], owned)
            copies.append(pltpu.make_async_copy(factors.at[at], outs[phase].at[s], sems.at[phase, s]))
            copies[-1].start()
    for copy in copies:
        copy.wait()


def integrals_body(phase, own, came, factors, arrived, keep, send, source, early):
    count, half, _ = keep.shape
    owned = factors.shape[0]
    mine, other = halves(half)
    for s in range(count):
        i, j, alone = phase_pair(phase, s, own, came)
        second = factors[lax.rem(j, owned)]
        first = early if s == count - 1 else source.at[s]
        first[...] = jnp.where(alone, factors[lax.rem(i, owned)], arrived[s])
        send[s] = nt_dot(first[pl.ds(other, half), :], second).astype(BF16)
        keep[s] = nt_dot(first[pl.ds(mine, half), :], second)


def chosen_integrals_body(seconds, source, keep, send):
    count, half, _ = keep.shape
    mine, other = halves(half)
    for s in range(count):
        send[s] = nt_dot(source[s, pl.ds(other, half), :], seconds[s]).astype(BF16)
        keep[s] = nt_dot(source[s, pl.ds(mine, half), :], seconds[s])


def add_body(held, came, total, send):
    total[...] = held[...] + came[...].astype(F32)
    send[...] = total[...].astype(BF16)


def facts_body(own, *refs):
    lists, (occ, column, row, factors), outs = refs[:2], refs[2:6], refs[6:8]
    seconds, alone_first = refs[8], refs[9:]
    count, half, _ = outs[0].shape
    owned = factors.shape[0]
    mine, _ = halves(half)
    for s in range(count):
        for phase in PHASES:
            i, j, alone = phase_pair(phase, s, own, lists[phase])
            outs[phase][s] = (occ[i] + occ[j]) - column[pl.ds(mine, half), :] - row[...]
        seconds[s] = factors[lax.rem(j, owned)]
        if alone_first:
            first = factors[lax.rem(i, owned)]
            alone_first[0][s] = jnp.where(alone, first, jnp.zeros_like(first))


def choose_body(phase, own, other_list, moved, out):
    for s in range(out.shape[0]):
        _, j, _ = phase_pair(phase, s, own, other_list)
        out[s] = moved[lax.rem(j, moved.shape[0])]


def amplitudes_body(denominators, held, came, out):
    out[...] = ((held[...] + came[...].astype(F32)) / denominators[...]).astype(BF16)


def terms_body(chosen, amps, came, back, whole):
    count, half, _ = amps.shape
    mine, other = halves(half)
    for s in range(count):
        whole[s, pl.ds(mine, half), :] = amps[s]
        whole[s, pl.ds(other, half), :] = came[s]
        back[s] = nn_dot(whole[s], chosen[s]).astype(BF16)


def density_body(source, whole, density):
    for s in range(density.shape[0]):
        density[s] = tn_dot(whole[s], source[s]).astype(BF16)


def metric_rows(metric, offset, width):
    start = jnp.bitwise_xor(lax.axis_index("aux"), offset) * width
    return metric[pl.ds(pl.multiple_of(start, width), width), :]


def moved_body(offsets, first, metric, *refs):
    out = refs[-1]
    blocks = refs[-1 - len(offsets) : -1]
    for o in range(out.shape[0]):
        total = None if first else refs[0][o]
        for offset, block in zip(offsets, blocks):
            term = nn_dot(block[o], metric_rows(metric, offset, block.shape[-1]))
            total = term if total is None else total + term
        out[o] = total.astype(out.dtype)


def moved_last_body(offset, phase, s, own, other_list, metric, held, block, out, picked, chosen):
    moved_body([offset], False, metric, held, block, out)
    right, _ = meeting(phase)
    picked[...] = out[lax.rem(own[0, 3 * s + 2 * right], out.shape[0])]
    choose_body(0, own, other_list, out, chosen)


def own_amplitudes_body(phase, own, other_list, occ, column, row, moved, *refs):
    blocks, out, chosen = refs[:-2], refs[-2], refs[-1]
    choose_body(phase, own, other_list, moved, chosen)
    count, half, _ = out.shape
    owned = blocks[0].shape[0]
    mine, _ = halves(half)
    for s in range(count):
        i, j = own[0, 3 * s + 1], own[1, 3 * s + 1]
        total = None
        for block in blocks:
            term = nt_dot(block[lax.rem(i, owned), pl.ds(mine, half), :], block[lax.rem(j, owned)])
            total = term if total is None else total + term
        denominator = (occ[i] + occ[j]) - column[pl.ds(mine, half), :] - row[...]
        out[s] = (total / denominator).astype(BF16)


def own_terms_body(own, moved, amps, came, out, whole):
    owned = moved.shape[0]
    count, half, _ = amps.shape
    mine, other = halves(half)
    out[...] = jnp.zeros_like(out)
    for s in range(count):
        whole[s, pl.ds(mine, half), :] = amps[s]
        whole[s, pl.ds(other, half), :] = came[s]
        i, j = lax.rem(own[0, 3 * s + 1], owned), lax.rem(own[1, 3 * s + 1], owned)
        out[i] += nn_dot(whole[s], moved[j])
        out[j] += tn_dot(whole[s], moved[i])


def last_pairs_body(early_at, late_at, own, early_list, late_list, held, moved, *refs):
    early_amps, late_amps, traded, metric = refs[:4]
    blocks, out = refs[4:-1], refs[-1]
    owned = moved.shape[0]
    total = None
    for offset, block in enumerate(blocks):
        term = nn_dot(block[...], metric_rows(metric, offset, block.shape[-1]))
        total = term if total is None else total + term
    _, j, _ = phase_pair(*early_at, own, early_list)
    out[lax.rem(j, owned)] += tn_dot(early_amps[early_at[1]], total.astype(BF16))
    i, j, alone = phase_pair(*late_at, own, late_list)
    first = jnp.where(alone, moved[lax.rem(i, owned)], traded[...])
    out[lax.rem(j, owned)] += tn_dot(late_amps[late_at[1]], first)


def result_body(plan, own, lists, held, metric, *refs):
    total = refs[-1]
    owned = held.shape[0]
    for phase, offsets, with_back in plan:
        blocks, refs = refs[: len(offsets)], refs[len(offsets) :]
        for s in range(blocks[0].shape[0]):
            _, j, _ = phase_pair(phase, s, own, lists[phase])
            term = None
            for offset, block in zip(offsets, blocks):
                part = nn_dot(block[s], metric_rows(metric, offset, block.shape[-1]))
                term = part if term is None else term + part
            total[lax.rem(j, owned)] += term
        if with_back:
            (back, came), refs = refs[:2], refs[2:]
            right, alone = meeting(phase)
            for s in range(back.shape[0]):
                at = lax.rem(own[0, 3 * s + 2 * right], owned)
                total[at] += jnp.where(alone, back[s], came[s]).astype(F32)


def result0_body(plan, own, list0, list1, held, metric, *refs):
    result_body(plan, own, (list0, list1), held, metric, *refs)


def result1_body(plan, own, list1, held, metric, *refs):
    *refs, back, code, total = refs
    result_body(plan, own, (None, list1), held, metric, *refs, total)
    owned = held.shape[0]
    right, alone = meeting(plan[0][0])
    number = jnp.int32(0)
    for s in range(back.shape[0]):
        at = lax.rem(own[0, 3 * s + 2 * right], owned)
        number = number + at * owned**s

        @pl.when(alone)
        def _():
            total[at] += back[s].astype(F32)

    code[...] = jnp.full(code.shape, number.astype(F32))


def last_body(held, code, came, out, total, staged, sems):
    owned = held.shape[0]
    number = jnp.max(code[...]).astype(jnp.int32)
    for s in range(came.shape[0]):
        total[lax.rem(number, owned)] += came[s].astype(F32)
        number = lax.div(number, owned)
    copies = [pltpu.make_async_copy(staged.at[o], out.at[o], sems.at[o]) for o in range(owned)]
    for o, copy in enumerate(copies):
        staged[o] = total[o].astype(BF16)
        copy.start()
    for copy in copies:
        copy.wait()


def flip(value, bit):
    size = lax.axis_size("aux")
    return lax.ppermute(value, "aux", [(k, k ^ (1 << bit)) for k in range(size)])


def meet(value, phase):
    size = lax.axis_size("orb")
    swaps = [(k, mate(k, phase)) for k in range(size) if 0 <= mate(k, phase) < size]
    return lax.ppermute(value, "orb", swaps)


def gathered(block, bits):
    blocks = {0: block}
    for bit in reversed(range(bits)):
        blocks.update({o ^ (1 << bit): flip(b, bit) for o, b in list(blocks.items())})
    return [blocks[o] for o in range(1 << bits)]


def local(orbital_factors, metric_factor, occ_energy, vir_energy, pair_list):
    owned, virtuals, width = orbital_factors.shape
    columns = metric_factor.shape[1]
    size = lax.axis_size("aux")
    bits = size.bit_length() - 1
    assert size == 1 << bits and bits >= 2
    count = pair_list.shape[0] // 3
    pair_list = pair_list.T
    half = virtuals // 2
    cube = 2 * virtuals * virtuals * width
    column = vir_energy[:, None]
    row = vir_energy[None, :]
    wide, narrow = (struct((count, half, virtuals), t) for t in (F32, BF16))

    sends = call(
        functools.partial(pick_body, count),
        [struct((count, virtuals, width), BF16)] * 2,
        [SM, pl.BlockSpec(memory_space=pltpu.HBM)],
        cube // 8,
        (pair_list, orbital_factors),
        [pltpu.SemaphoreType.DMA((2, count))],
    )
    arrived = [meet(sends[x], x) for x in PHASES]
    lists = [meet(pair_list, x) for x in PHASES]
    blocks = gathered(orbital_factors, bits)
    shape = (owned, virtuals, columns)
    wave = cube * owned
    low = [o for o in range(size) if o < 2]
    moved = call(
        functools.partial(moved_body, low, True),
        struct(shape, F32),
        [VM] * 3,
        2 * wave,
        (metric_factor, *[blocks[o] for o in low]),
    )
    for o in range(2, size - 1):
        moved = call(
            functools.partial(moved_body, [o], False),
            struct(shape, F32),
            [VM] * 3,
            wave,
            (metric_factor, moved, blocks[o]),
            alias={1: 0},
        )
    direct = count - 1
    some = struct((count, virtuals, columns), BF16)
    moved, picked, chosen = call(
        functools.partial(moved_last_body, size - 1, PHASES[-1], direct),
        [struct(shape, BF16), struct((virtuals, columns), BF16), some],
        [SM] * 2 + [VM] * 3,
        wave,
        (pair_list, lists[0], metric_factor, moved, blocks[size - 1]),
    )
    traded = meet(picked, PHASES[-1])

    late, last = PHASES[-1], count - 1
    some = struct((count, virtuals, width), BF16)
    rest = struct((last, virtuals, width), BF16)
    lonely = lax.axis_size("orb") % 2 == 1
    keep0, send0, source0, early = call(
        functools.partial(integrals_body, 0),
        [wide, narrow, rest, struct((virtuals, width), BF16)],
        [SM] * 2 + [VM] * 2,
        count * cube,
        (pair_list, lists[0], orbital_factors, arrived[0]),
    )
    *denominators, seconds, alone_first = call(
        facts_body,
        [wide, wide, some] + [some] * lonely,
        [SM] * 4 + [VM] * 3,
        cube // 8,
        (pair_list, *lists, occ_energy, column, row, orbital_factors),
    ) + [None] * (not lonely)
    source1 = arrived[1] + alone_first if lonely else arrived[1]
    keep1, send1 = call(chosen_integrals_body, [wide, narrow], [VM] * 2, count * cube, (seconds, source1))
    sums = [(keep0, send0), (keep1, send1)]
    sources = [source0, source1]
    early_blocks = gathered(early, bits)

    wholes, gathers = [], []
    for x in PHASES:
        keep, send = sums[x]
        for bit in range(bits - 1):
            keep, send = call(add_body, [wide, narrow], [VM] * 2, cube // 8, (keep, flip(send, bit)))
        amps = call(amplitudes_body, narrow, [VM] * 3, cube // 8, (denominators[x], keep, flip(send, bits - 1)))
        if x == late:
            own_amps, chosen = call(
                functools.partial(own_amplitudes_body, x),
                [narrow, struct((count, virtuals, columns), BF16)],
                [SM] * 3 + [VM] * (3 + size),
                cube * count * size // 2,
                (pair_list, lists[x], occ_energy, column, row, moved, *blocks),
            )
        back, whole = call(
            terms_body,
            [struct((count, virtuals, columns), BF16), struct((count, virtuals, virtuals), BF16)],
            [VM] * 3,
            count * cube,
            (chosen, amps, flip(amps, 0)),
        )
        density = call(density_body, rest, [VM] * 2, last * cube, (sources[x], whole))
        wholes.append(whole)
        gathers.append((gathered(density, bits), back, meet(back, x)))

    held = call(
        own_terms_body,
        struct(shape, F32),
        [SM] + [VM] * 3,
        2 * count * cube,
        (pair_list, moved, own_amps, flip(own_amps, 0)),
        [pltpu.VMEM((count, virtuals, virtuals), BF16)],
    )
    held = call(
        functools.partial(last_pairs_body, (0, last), (late, direct)),
        struct(shape, F32),
        [SM] * 3 + [VM] * (6 + size),
        cube,
        (pair_list, *lists, held, moved, *wholes, traded, metric_factor, *early_blocks),
        alias={3: 0},
    )
    (blocks0, back0, came0), (blocks1, back1, came1) = gathers
    held = call(
        functools.partial(result0_body, [(0, range(size), True), (1, low, False)]),
        struct(shape, F32),
        [SM] * 3 + [VM] * (4 + size + len(low)),
        (size + 2) * last * cube,
        (pair_list, *lists, held, metric_factor, *blocks0, back0, came0, *[blocks1[o] for o in low]),
        alias={3: 0},
    )
    high = range(2, size)
    code, held = call(
        functools.partial(result1_body, [(1, high, False)]),
        [struct((8, 128), F32), struct(shape, F32)],
        [SM] * 2 + [VM] * (3 + len(high)),
        last * len(high) * cube,
        (pair_list, lists[1], held, metric_factor, *[blocks1[o] for o in high], back1),
        alias={2: 1},
    )
    return call(
        last_body,
        [struct(shape, BF16), struct(shape, F32)],
        [VM] * 3,
        cube // 8,
        (held, code, came1),
        [pltpu.VMEM(shape, BF16), pltpu.SemaphoreType.DMA((owned,))],
        alias={0: 1},
        out_specs=[pl.BlockSpec(memory_space=pltpu.HBM), VM],
    )[0]


def solution(mesh):
    placed = (P("orb", None, "aux"), P(None, "aux"), P(), P(), P("orb", None))
    return jax.shard_map(local, mesh=mesh, in_specs=placed, out_specs=P("orb", None, "aux"), check_vma=False)
```

```python
import functools

import jax
import jax.numpy as jnp
from jax import lax
from jax.experimental import pallas as pl
from jax.experimental.pallas import tpu as pltpu
from jax.sharding import PartitionSpec as P


F32 = jnp.float32
BF16 = jnp.bfloat16
VM = pl.BlockSpec(memory_space=pltpu.VMEM)
SM = pl.BlockSpec(memory_space=pltpu.SMEM)
PHASES = (0, 1)


def struct(shape, dtype):
    return jax.ShapeDtypeStruct(shape, dtype)


def call(body, outs, in_specs, flops, args, scratch=(), limit=16, alias=None, out_specs=None):
    moved = sum(a.size * a.dtype.itemsize for a in args)
    done = pl.pallas_call(
        body,
        out_shape=outs,
        in_specs=in_specs,
        out_specs=out_specs or jax.tree.map(lambda _: VM, outs),
        scratch_shapes=scratch,
        input_output_aliases=alias or {},
        compiler_params=pltpu.CompilerParams(vmem_limit_bytes=limit << 20),
        cost_estimate=pl.CostEstimate(flops=int(flops), bytes_accessed=int(moved), transcendentals=0),
    )(*args)
    return list(done) if isinstance(done, tuple) else done


def mate(place, phase):
    return ((place + 1 - phase) ^ 1) - 1 + phase


def meeting(phase):
    g = lax.axis_index("orb")
    right = jnp.bitwise_and(g + phase, 1)
    other = g + 2 * right - 1
    return right, jnp.logical_or(other < 0, other >= lax.axis_size("orb"))


def phase_pair(phase, s, own, came):
    right, alone = meeting(phase)
    i, j = [jnp.where(alone, own[c, 3 * s + 2 * right], came[c, 3 * s + 2 * (1 - right)]) for c in (0, 1)]
    return i, j, alone


def nt_dot(a, b):
    return lax.dot_general(a, b, (((1,), (1,)), ((), ())), preferred_element_type=F32)


def tn_dot(a, b):
    return lax.dot_general(a, b, (((0,), (0,)), ((), ())), preferred_element_type=F32)


def nn_dot(a, b):
    return lax.dot_general(a, b, (((1,), (0,)), ((), ())), preferred_element_type=F32)


def halves(half):
    mine = jnp.bitwise_and(lax.axis_index("aux"), 1)
    return pl.multiple_of(mine * half, half), pl.multiple_of((1 - mine) * half, half)


def pick_body(count, own, factors, *refs):
    outs, sems = refs[:-1], refs[-1]
    owned = factors.shape[0]
    copies = []
    for phase in PHASES:
        right, _ = meeting(phase)
        for s in range(count):
            at = lax.rem(own[0, 3 * s + 2 * right], owned)
            copies.append(pltpu.make_async_copy(factors.at[at], outs[phase].at[s], sems.at[phase, s]))
            copies[-1].start()
    for copy in copies:
        copy.wait()


def integrals_body(phase, own, came, factors, arrived, keep, send, source, early):
    count, half, _ = keep.shape
    owned = factors.shape[0]
    mine, other = halves(half)
    for s in range(count):
        i, j, alone = phase_pair(phase, s, own, came)
        second = factors[lax.rem(j, owned)]
        first = early if s == count - 1 else source.at[s]
        first[...] = jnp.where(alone, factors[lax.rem(i, owned)], arrived[s])
        send[s] = nt_dot(first[pl.ds(other, half), :], second).astype(BF16)
        keep[s] = nt_dot(first[pl.ds(mine, half), :], second)


def chosen_integrals_body(seconds, source, keep, send):
    count, half, _ = keep.shape
    mine, other = halves(half)
    for s in range(count):
        send[s] = nt_dot(source[s, pl.ds(other, half), :], seconds[s]).astype(BF16)
        keep[s] = nt_dot(source[s, pl.ds(mine, half), :], seconds[s])


def add_body(held, came, total, send):
    total[...] = held[...] + came[...].astype(F32)
    send[...] = total[...].astype(BF16)


def add_apart_body(held, came, total, *sends):
    total[...] = held[...] + came[...].astype(F32)
    for s, send in enumerate(sends):
        send[...] = total[s].astype(BF16)


def facts_body(own, *refs):
    lists, (occ, column, row, factors), outs = refs[:2], refs[2:6], refs[6:8]
    seconds, alone_first = refs[8], refs[9:]
    count, half, _ = outs[0].shape
    owned = factors.shape[0]
    mine, _ = halves(half)
    for s in range(count):
        for phase in PHASES:
            i, j, alone = phase_pair(phase, s, own, lists[phase])
            outs[phase][s] = (occ[i] + occ[j]) - column[pl.ds(mine, half), :] - row[...]
        seconds[s] = factors[lax.rem(j, owned)]
        if alone_first:
            first = factors[lax.rem(i, owned)]
            alone_first[0][s] = jnp.where(alone, first, jnp.zeros_like(first))


def choose_body(phase, own, other_list, moved, out):
    for s in range(out.shape[0]):
        _, j, _ = phase_pair(phase, s, own, other_list)
        out[s] = moved[lax.rem(j, moved.shape[0])]


def amplitudes_body(denominators, held, came, out):
    out[...] = ((held[...] + came[...].astype(F32)) / denominators[...]).astype(BF16)


def pair_amplitudes_body(s, denominators, held, came, out):
    out[...] = ((held[s] + came[...].astype(F32)) / denominators[s]).astype(BF16)


def pair_terms_body(s, chosen, amps, came, back, whole):
    half = amps.shape[0]
    mine, other = halves(half)
    whole[pl.ds(mine, half), :] = amps[...]
    whole[pl.ds(other, half), :] = came[...]
    back[...] = nn_dot(whole[...], chosen[s]).astype(BF16)


def pair_density_body(source, *refs):
    wholes, density = refs[:-1], refs[-1]
    for s, whole in enumerate(wholes):
        density[s] = tn_dot(whole[...], source[s]).astype(BF16)


def terms_body(chosen, amps, came, back, whole):
    count, half, _ = amps.shape
    mine, other = halves(half)
    for s in range(count):
        whole[s, pl.ds(mine, half), :] = amps[s]
        whole[s, pl.ds(other, half), :] = came[s]
        back[s] = nn_dot(whole[s], chosen[s]).astype(BF16)


def density_body(source, whole, density):
    for s in range(density.shape[0]):
        density[s] = tn_dot(whole[s], source[s]).astype(BF16)


def metric_rows(metric, offset, width):
    start = jnp.bitwise_xor(lax.axis_index("aux"), offset) * width
    return metric[pl.ds(pl.multiple_of(start, width), width), :]


def moved_body(offsets, first, metric, *refs):
    out = refs[-1]
    blocks = refs[-1 - len(offsets) : -1]
    for o in range(out.shape[0]):
        total = None if first else refs[0][o]
        for offset, block in zip(offsets, blocks):
            term = nn_dot(block[o], metric_rows(metric, offset, block.shape[-1]))
            total = term if total is None else total + term
        out[o] = total.astype(out.dtype)


def moved_last_body(offset, phase, s, own, other_list, metric, held, block, out, picked, chosen):
    moved_body([offset], False, metric, held, block, out)
    right, _ = meeting(phase)
    picked[...] = out[lax.rem(own[0, 3 * s + 2 * right], out.shape[0])]
    choose_body(0, own, other_list, out, chosen)


def own_amplitudes_body(phase, own, other_list, occ, column, row, moved, *refs):
    blocks, out, chosen = refs[:-2], refs[-2], refs[-1]
    choose_body(phase, own, other_list, moved, chosen)
    count, half, _ = out.shape
    owned = blocks[0].shape[0]
    mine, _ = halves(half)
    for s in range(count):
        i, j = own[0, 3 * s + 1], own[1, 3 * s + 1]
        total = None
        for block in blocks:
            term = nt_dot(block[lax.rem(i, owned), pl.ds(mine, half), :], block[lax.rem(j, owned)])
            total = term if total is None else total + term
        denominator = (occ[i] + occ[j]) - column[pl.ds(mine, half), :] - row[...]
        out[s] = (total / denominator).astype(BF16)


def own_terms_body(own, moved, amps, came, out, whole):
    owned = moved.shape[0]
    count, half, _ = amps.shape
    mine, other = halves(half)
    out[...] = jnp.zeros_like(out)
    for s in range(count):
        whole[s, pl.ds(mine, half), :] = amps[s]
        whole[s, pl.ds(other, half), :] = came[s]
        i, j = lax.rem(own[0, 3 * s + 1], owned), lax.rem(own[1, 3 * s + 1], owned)
        out[i] += nn_dot(whole[s], moved[j])
        out[j] += tn_dot(whole[s], moved[i])


def last_pairs_body(early_at, late_at, own, early_list, late_list, held, moved, *refs):
    early_amps, late_amps, traded, metric = refs[:4]
    blocks, out = refs[4:-1], refs[-1]
    owned = moved.shape[0]
    total = None
    for offset, block in enumerate(blocks):
        term = nn_dot(block[...], metric_rows(metric, offset, block.shape[-1]))
        total = term if total is None else total + term
    _, j, _ = phase_pair(*early_at, own, early_list)
    out[lax.rem(j, owned)] += tn_dot(early_amps[early_at[1]], total.astype(BF16))
    i, j, alone = phase_pair(*late_at, own, late_list)
    first = jnp.where(alone, moved[lax.rem(i, owned)], traded[...])
    out[lax.rem(j, owned)] += tn_dot(late_amps[...], first)


def result_body(plan, own, lists, held, metric, *refs):
    total = refs[-1]
    owned = held.shape[0]
    for phase, offsets, with_back in plan:
        blocks, refs = refs[: len(offsets)], refs[len(offsets) :]
        for s in range(blocks[0].shape[0]):
            _, j, _ = phase_pair(phase, s, own, lists[phase])
            term = None
            for offset, block in zip(offsets, blocks):
                part = nn_dot(block[s], metric_rows(metric, offset, block.shape[-1]))
                term = part if term is None else term + part
            total[lax.rem(j, owned)] += term
        if with_back:
            (back, came), refs = refs[:2], refs[2:]
            right, alone = meeting(phase)
            for s in range(back.shape[0]):
                at = lax.rem(own[0, 3 * s + 2 * right], owned)
                total[at] += jnp.where(alone, back[s], came[s]).astype(F32)


def result0_body(plan, own, list0, list1, held, metric, *refs):
    result_body(plan, own, (list0, list1), held, metric, *refs)


def result1_body(plan, count, own, list1, held, metric, *refs):
    *refs, code, total = refs
    cames, refs = refs[1 - count :], refs[: 1 - count]
    backs, refs = refs[-count:], refs[:-count]
    result_body(plan, own, (None, list1), held, metric, *refs, total)
    owned = held.shape[0]
    right, alone = meeting(plan[0][0])
    for s in range(count):
        at = lax.rem(own[0, 3 * s + 2 * right], owned)
        if s < count - 1:
            total[at] += jnp.where(alone, backs[s][...], cames[s][...]).astype(F32)
    code[...] = jnp.full(code.shape, at.astype(F32))

    @pl.when(alone)
    def _():
        total[at] += backs[count - 1][...].astype(F32)


def last_body(held, code, came, out, total, staged, sems):
    owned = held.shape[0]
    total[jnp.max(code[...]).astype(jnp.int32)] += came[...].astype(F32)
    copies = [pltpu.make_async_copy(staged.at[o], out.at[o], sems.at[o]) for o in range(owned)]
    for o, copy in enumerate(copies):
        staged[o] = total[o].astype(BF16)
        copy.start()
    for copy in copies:
        copy.wait()


def flip(value, bit):
    size = lax.axis_size("aux")
    return lax.ppermute(value, "aux", [(k, k ^ (1 << bit)) for k in range(size)])


def meet(value, phase):
    size = lax.axis_size("orb")
    swaps = [(k, mate(k, phase)) for k in range(size) if 0 <= mate(k, phase) < size]
    return lax.ppermute(value, "orb", swaps)


def gathered(block, bits):
    blocks = {0: block}
    for bit in reversed(range(bits)):
        blocks.update({o ^ (1 << bit): flip(b, bit) for o, b in list(blocks.items())})
    return [blocks[o] for o in range(1 << bits)]


def local(orbital_factors, metric_factor, occ_energy, vir_energy, pair_list):
    owned, virtuals, width = orbital_factors.shape
    columns = metric_factor.shape[1]
    size = lax.axis_size("aux")
    bits = size.bit_length() - 1
    assert size == 1 << bits and bits >= 2
    count = pair_list.shape[0] // 3
    pair_list = pair_list.T
    half = virtuals // 2
    cube = 2 * virtuals * virtuals * width
    column = vir_energy[:, None]
    row = vir_energy[None, :]
    wide, narrow = (struct((count, half, virtuals), t) for t in (F32, BF16))

    sends = call(
        functools.partial(pick_body, count),
        [struct((count, virtuals, width), BF16)] * 2,
        [SM, pl.BlockSpec(memory_space=pltpu.HBM)],
        cube // 8,
        (pair_list, orbital_factors),
        [pltpu.SemaphoreType.DMA((2, count))],
    )
    arrived = [meet(sends[x], x) for x in PHASES]
    lists = [meet(pair_list, x) for x in PHASES]
    blocks = gathered(orbital_factors, bits)
    shape = (owned, virtuals, columns)
    wave = cube * owned
    low = [o for o in range(size) if o < 2]
    moved = call(
        functools.partial(moved_body, low, True),
        struct(shape, F32),
        [VM] * 3,
        2 * wave,
        (metric_factor, *[blocks[o] for o in low]),
    )
    for o in range(2, size - 1):
        moved = call(
            functools.partial(moved_body, [o], False),
            struct(shape, F32),
            [VM] * 3,
            wave,
            (metric_factor, moved, blocks[o]),
            alias={1: 0},
        )
    direct = count - 1
    some = struct((count, virtuals, columns), BF16)
    moved, picked, chosen = call(
        functools.partial(moved_last_body, size - 1, PHASES[-1], direct),
        [struct(shape, BF16), struct((virtuals, columns), BF16), some],
        [SM] * 2 + [VM] * 3,
        wave,
        (pair_list, lists[0], metric_factor, moved, blocks[size - 1]),
    )
    traded = meet(picked, PHASES[-1])

    late, last = PHASES[-1], count - 1
    some = struct((count, virtuals, width), BF16)
    rest = struct((last, virtuals, width), BF16)
    lonely = lax.axis_size("orb") % 2 == 1
    keep0, send0, source0, early = call(
        functools.partial(integrals_body, 0),
        [wide, narrow, rest, struct((virtuals, width), BF16)],
        [SM] * 2 + [VM] * 2,
        count * cube,
        (pair_list, lists[0], orbital_factors, arrived[0]),
    )
    *denominators, seconds, alone_first = call(
        facts_body,
        [wide, wide, some] + [some] * lonely,
        [SM] * 4 + [VM] * 3,
        cube // 8,
        (pair_list, *lists, occ_energy, column, row, orbital_factors),
    ) + [None] * (not lonely)
    source1 = arrived[1] + alone_first if lonely else arrived[1]
    keep1, send1 = call(chosen_integrals_body, [wide, narrow], [VM] * 2, count * cube, (seconds, source1))
    early_blocks = gathered(early, bits)

    keep, send = keep0, send0
    for bit in range(bits - 1):
        keep, send = call(add_body, [wide, narrow], [VM] * 2, cube // 8, (keep, flip(send, bit)))
    amps = call(amplitudes_body, narrow, [VM] * 3, cube // 8, (denominators[0], keep, flip(send, bits - 1)))
    back0, whole0 = call(
        terms_body,
        [struct((count, virtuals, columns), BF16), struct((count, virtuals, virtuals), BF16)],
        [VM] * 3,
        count * cube,
        (chosen, amps, flip(amps, 0)),
    )
    density0 = call(density_body, rest, [VM] * 2, last * cube, (source0, whole0))
    came0 = meet(back0, 0)
    blocks0 = gathered(density0, bits)

    own_amps, chosen = call(
        functools.partial(own_amplitudes_body, late),
        [narrow, struct((count, virtuals, columns), BF16)],
        [SM] * 3 + [VM] * (3 + size),
        cube * count * size // 2,
        (pair_list, lists[late], occ_energy, column, row, moved, *blocks),
    )
    keep, send = keep1, send1
    for bit in range(bits - 2):
        keep, send = call(add_body, [wide, narrow], [VM] * 2, cube // 8, (keep, flip(send, bit)))
    piece = struct((half, virtuals), BF16)
    keep, *sends = call(add_apart_body, [wide] + [piece] * count, [VM] * 2, cube // 8, (keep, flip(send, bits - 2)))
    wholes, backs, cames = [], [], []
    for s in range(count):
        amps = call(
            functools.partial(pair_amplitudes_body, s),
            piece,
            [VM] * 3,
            cube // 16,
            (denominators[1], keep, flip(sends[s], bits - 1)),
        )
        back, whole = call(
            functools.partial(pair_terms_body, s),
            [struct((virtuals, columns), BF16), struct((virtuals, virtuals), BF16)],
            [VM] * 3,
            cube,
            (chosen, amps, flip(amps, 0)),
        )
        wholes.append(whole)
        backs.append(back)
        cames.append(meet(back, late))
    density1 = call(pair_density_body, rest, [VM] * count, last * cube, (source1, *wholes[:last]))
    blocks1 = gathered(density1, bits)

    held = call(
        own_terms_body,
        struct(shape, F32),
        [SM] + [VM] * 3,
        2 * count * cube,
        (pair_list, moved, own_amps, flip(own_amps, 0)),
        [pltpu.VMEM((count, virtuals, virtuals), BF16)],
    )
    held = call(
        functools.partial(last_pairs_body, (0, last), (late, direct)),
        struct(shape, F32),
        [SM] * 3 + [VM] * (6 + size),
        cube,
        (pair_list, *lists, held, moved, whole0, wholes[last], traded, metric_factor, *early_blocks),
        alias={3: 0},
    )
    held = call(
        functools.partial(result0_body, [(0, range(size), True), (1, low, False)]),
        struct(shape, F32),
        [SM] * 3 + [VM] * (4 + size + len(low)),
        (size + 2) * last * cube,
        (pair_list, *lists, held, metric_factor, *blocks0, back0, came0, *[blocks1[o] for o in low]),
        alias={3: 0},
    )
    high = range(2, size)
    code, held = call(
        functools.partial(result1_body, [(1, high, False)], count),
        [struct((8, 128), F32), struct(shape, F32)],
        [SM] * 2 + [VM] * (1 + len(high) + 2 * count),
        last * len(high) * cube,
        (pair_list, lists[1], held, metric_factor, *[blocks1[o] for o in high], *backs, *cames[:last]),
        alias={2: 1},
    )
    return call(
        last_body,
        [struct(shape, BF16), struct(shape, F32)],
        [VM] * 3,
        cube // 8,
        (held, code, cames[last]),
        [pltpu.VMEM(shape, BF16), pltpu.SemaphoreType.DMA((owned,))],
        alias={0: 1},
        out_specs=[pl.BlockSpec(memory_space=pltpu.HBM), VM],
    )[0]


def solution(mesh):
    placed = (P("orb", None, "aux"), P(None, "aux"), P(), P(), P("orb", None))
    return jax.shard_map(local, mesh=mesh, in_specs=placed, out_specs=P("orb", None, "aux"), check_vma=False)
```

```python
import functools

import jax
import jax.numpy as jnp
from jax import lax
from jax.experimental import pallas as pl
from jax.experimental.pallas import tpu as pltpu
from jax.sharding import PartitionSpec as P


F32 = jnp.float32
BF16 = jnp.bfloat16
VM = pl.BlockSpec(memory_space=pltpu.VMEM)
SM = pl.BlockSpec(memory_space=pltpu.SMEM)
PHASES = (0, 1)


def struct(shape, dtype):
    return jax.ShapeDtypeStruct(shape, dtype)


def call(body, outs, in_specs, flops, args, scratch=(), limit=16, alias=None, out_specs=None):
    moved = sum(a.size * a.dtype.itemsize for a in args)
    done = pl.pallas_call(
        body,
        out_shape=outs,
        in_specs=in_specs,
        out_specs=out_specs or jax.tree.map(lambda _: VM, outs),
        scratch_shapes=scratch,
        input_output_aliases=alias or {},
        compiler_params=pltpu.CompilerParams(vmem_limit_bytes=limit << 20),
        cost_estimate=pl.CostEstimate(flops=int(flops), bytes_accessed=int(moved), transcendentals=0),
    )(*args)
    return list(done) if isinstance(done, tuple) else done


def mate(place, phase):
    return ((place + 1 - phase) ^ 1) - 1 + phase


def meeting(phase):
    g = lax.axis_index("orb")
    right = jnp.bitwise_and(g + phase, 1)
    other = g + 2 * right - 1
    return right, jnp.logical_or(other < 0, other >= lax.axis_size("orb"))


def phase_pair(phase, s, own, came):
    right, alone = meeting(phase)
    i, j = [jnp.where(alone, own[c, 3 * s + 2 * right], came[c, 3 * s + 2 * (1 - right)]) for c in (0, 1)]
    return i, j, alone


def nt_dot(a, b):
    return lax.dot_general(a, b, (((1,), (1,)), ((), ())), preferred_element_type=F32)


def tn_dot(a, b):
    return lax.dot_general(a, b, (((0,), (0,)), ((), ())), preferred_element_type=F32)


def nn_dot(a, b):
    return lax.dot_general(a, b, (((1,), (0,)), ((), ())), preferred_element_type=F32)


def halves(half):
    mine = jnp.bitwise_and(lax.axis_index("aux"), 1)
    return pl.multiple_of(mine * half, half), pl.multiple_of((1 - mine) * half, half)


def pick_body(count, own, factors, *refs):
    outs, sems = refs[:-1], refs[-1]
    owned = factors.shape[0]
    copies = []
    for phase in PHASES:
        right, _ = meeting(phase)
        for s in range(count):
            at = lax.rem(own[0, 3 * s + 2 * right], owned)
            copies.append(pltpu.make_async_copy(factors.at[at], outs[phase].at[s], sems.at[phase, s]))
            copies[-1].start()
    for copy in copies:
        copy.wait()


def integrals_body(phase, own, came, factors, arrived, keep, send, source, early):
    count, half, _ = keep.shape
    owned = factors.shape[0]
    mine, other = halves(half)
    for s in range(count):
        i, j, alone = phase_pair(phase, s, own, came)
        second = factors[lax.rem(j, owned)]
        first = early if s == count - 1 else source.at[s]
        first[...] = jnp.where(alone, factors[lax.rem(i, owned)], arrived[s])
        send[s] = nt_dot(first[pl.ds(other, half), :], second).astype(BF16)
        keep[s] = nt_dot(first[pl.ds(mine, half), :], second)


def chosen_integrals_body(seconds, source, keep, send):
    count, half, _ = keep.shape
    mine, other = halves(half)
    for s in range(count):
        send[s] = nt_dot(source[s, pl.ds(other, half), :], seconds[s]).astype(BF16)
        keep[s] = nt_dot(source[s, pl.ds(mine, half), :], seconds[s])


def add_body(held, came, total, send):
    total[...] = held[...] + came[...].astype(F32)
    send[...] = total[...].astype(BF16)


def add_apart_body(held, came, total, *sends):
    total[...] = held[...] + came[...].astype(F32)
    for s, send in enumerate(sends):
        send[...] = total[s].astype(BF16)


def facts_body(own, *refs):
    lists, (occ, column, row, factors), outs = refs[:2], refs[2:6], refs[6:8]
    seconds, number, alone_first = refs[8], refs[9], refs[10:]
    count, half, _ = outs[0].shape
    owned = factors.shape[0]
    mine, _ = halves(half)
    for s in range(count):
        for phase in PHASES:
            i, j, alone = phase_pair(phase, s, own, lists[phase])
            outs[phase][s] = (occ[i] + occ[j]) - column[pl.ds(mine, half), :] - row[...]
        seconds[s] = factors[lax.rem(j, owned)]
        if alone_first:
            first = factors[lax.rem(i, owned)]
            alone_first[0][s] = jnp.where(alone, first, jnp.zeros_like(first))
    right, _ = meeting(PHASES[-1])
    total, weight = lax.rem(own[0, 3 * (count - 1) + 2 * right], owned), owned
    for s in range(count):
        _, j, _ = phase_pair(0, s, own, lists[0])
        total, weight = total + lax.rem(j, owned) * weight, weight * owned
    number[...] = jnp.full(number.shape, total.astype(F32))


def choose_body(phase, own, other_list, moved, out):
    for s in range(out.shape[0]):
        _, j, _ = phase_pair(phase, s, own, other_list)
        out[s] = moved[lax.rem(j, moved.shape[0])]


def amplitudes_body(denominators, held, came, out):
    out[...] = ((held[...] + came[...].astype(F32)) / denominators[...]).astype(BF16)


def pair_amplitudes_body(s, denominators, held, came, out):
    out[...] = ((held[s] + came[...].astype(F32)) / denominators[s]).astype(BF16)


def pair_terms_body(s, chosen, amps, came, back, whole):
    half = amps.shape[0]
    mine, other = halves(half)
    whole[pl.ds(mine, half), :] = amps[...]
    whole[pl.ds(other, half), :] = came[...]
    back[...] = nn_dot(whole[...], chosen[s]).astype(BF16)


def pair_density_body(source, *refs):
    wholes, density = refs[:-1], refs[-1]
    for s, whole in enumerate(wholes):
        density[s] = tn_dot(whole[...], source[s]).astype(BF16)


def terms_body(chosen, amps, came, back, whole):
    count, half, _ = amps.shape
    mine, other = halves(half)
    for s in range(count):
        whole[s, pl.ds(mine, half), :] = amps[s]
        whole[s, pl.ds(other, half), :] = came[s]
        back[s] = nn_dot(whole[s], chosen[s]).astype(BF16)


def density_body(source, whole, density):
    for s in range(density.shape[0]):
        density[s] = tn_dot(whole[s], source[s]).astype(BF16)


def metric_rows(metric, offset, width):
    start = jnp.bitwise_xor(lax.axis_index("aux"), offset) * width
    return metric[pl.ds(pl.multiple_of(start, width), width), :]


def moved_body(offsets, first, metric, *refs):
    out = refs[-1]
    blocks = refs[-1 - len(offsets) : -1]
    for o in range(out.shape[0]):
        total = None if first else refs[0][o]
        for offset, block in zip(offsets, blocks):
            term = nn_dot(block[o], metric_rows(metric, offset, block.shape[-1]))
            total = term if total is None else total + term
        out[o] = total.astype(out.dtype)


def moved_last_body(offset, metric, held, block, number, out, picked, chosen):
    moved_body([offset], False, metric, held, block, out)
    owned = out.shape[0]
    rest = jnp.max(number[...]).astype(jnp.int32)
    picked[...] = out[lax.rem(rest, owned)]
    for s in range(chosen.shape[0]):
        rest = lax.div(rest, owned)
        chosen[s] = out[lax.rem(rest, owned)]


def own_amplitudes_body(phase, own, other_list, occ, column, row, moved, *refs):
    blocks, out, chosen = refs[:-2], refs[-2], refs[-1]
    choose_body(phase, own, other_list, moved, chosen)
    count, half, _ = out.shape
    owned = blocks[0].shape[0]
    mine, _ = halves(half)
    for s in range(count):
        i, j = own[0, 3 * s + 1], own[1, 3 * s + 1]
        total = None
        for block in blocks:
            term = nt_dot(block[lax.rem(i, owned), pl.ds(mine, half), :], block[lax.rem(j, owned)])
            total = term if total is None else total + term
        denominator = (occ[i] + occ[j]) - column[pl.ds(mine, half), :] - row[...]
        out[s] = (total / denominator).astype(BF16)


def own_terms_body(own, moved, amps, came, out, whole):
    owned = moved.shape[0]
    count, half, _ = amps.shape
    mine, other = halves(half)
    out[...] = jnp.zeros_like(out)
    for s in range(count):
        whole[s, pl.ds(mine, half), :] = amps[s]
        whole[s, pl.ds(other, half), :] = came[s]
        i, j = lax.rem(own[0, 3 * s + 1], owned), lax.rem(own[1, 3 * s + 1], owned)
        out[i] += nn_dot(whole[s], moved[j])
        out[j] += tn_dot(whole[s], moved[i])


def last_pairs_body(early_at, late_at, own, early_list, late_list, held, moved, *refs):
    early_amps, late_amps, traded, metric = refs[:4]
    blocks, out = refs[4:-1], refs[-1]
    owned = moved.shape[0]
    total = None
    for offset, block in enumerate(blocks):
        term = nn_dot(block[...], metric_rows(metric, offset, block.shape[-1]))
        total = term if total is None else total + term
    _, j, _ = phase_pair(*early_at, own, early_list)
    out[lax.rem(j, owned)] += tn_dot(early_amps[early_at[1]], total.astype(BF16))
    i, j, alone = phase_pair(*late_at, own, late_list)
    first = jnp.where(alone, moved[lax.rem(i, owned)], traded[...])
    out[lax.rem(j, owned)] += tn_dot(late_amps[...], first)


def result_body(plan, own, lists, held, metric, *refs):
    total = refs[-1]
    owned = held.shape[0]
    for phase, offsets, with_back in plan:
        blocks, refs = refs[: len(offsets)], refs[len(offsets) :]
        for s in range(blocks[0].shape[0]):
            _, j, _ = phase_pair(phase, s, own, lists[phase])
            term = None
            for offset, block in zip(offsets, blocks):
                part = nn_dot(block[s], metric_rows(metric, offset, block.shape[-1]))
                term = part if term is None else term + part
            total[lax.rem(j, owned)] += term
        if with_back:
            (back, came), refs = refs[:2], refs[2:]
            right, alone = meeting(phase)
            for s in range(back.shape[0]):
                at = lax.rem(own[0, 3 * s + 2 * right], owned)
                total[at] += jnp.where(alone, back[s], came[s]).astype(F32)


def result0_body(plan, own, list0, list1, held, metric, *refs):
    result_body(plan, own, (list0, list1), held, metric, *refs)


def result1_body(plan, count, own, list1, held, metric, *refs):
    *refs, code, total = refs
    cames, refs = refs[1 - count :], refs[: 1 - count]
    backs, refs = refs[-count:], refs[:-count]
    result_body(plan, own, (None, list1), held, metric, *refs, total)
    owned = held.shape[0]
    right, alone = meeting(plan[0][0])
    for s in range(count):
        at = lax.rem(own[0, 3 * s + 2 * right], owned)
        if s < count - 1:
            total[at] += jnp.where(alone, backs[s][...], cames[s][...]).astype(F32)
    code[...] = jnp.full(code.shape, at.astype(F32))

    @pl.when(alone)
    def _():
        total[at] += backs[count - 1][...].astype(F32)


def last_body(held, code, came, out, total, staged, sems):
    owned = held.shape[0]
    total[jnp.max(code[...]).astype(jnp.int32)] += came[...].astype(F32)
    copies = [pltpu.make_async_copy(staged.at[o], out.at[o], sems.at[o]) for o in range(owned)]
    for o, copy in enumerate(copies):
        staged[o] = total[o].astype(BF16)
        copy.start()
    for copy in copies:
        copy.wait()


def flip(value, bit):
    size = lax.axis_size("aux")
    return lax.ppermute(value, "aux", [(k, k ^ (1 << bit)) for k in range(size)])


def meet(value, phase):
    size = lax.axis_size("orb")
    swaps = [(k, mate(k, phase)) for k in range(size) if 0 <= mate(k, phase) < size]
    return lax.ppermute(value, "orb", swaps)


def gathered(block, bits):
    blocks = {0: block}
    for bit in reversed(range(bits)):
        blocks.update({o ^ (1 << bit): flip(b, bit) for o, b in list(blocks.items())})
    return [blocks[o] for o in range(1 << bits)]


def local(orbital_factors, metric_factor, occ_energy, vir_energy, pair_list):
    owned, virtuals, width = orbital_factors.shape
    columns = metric_factor.shape[1]
    size = lax.axis_size("aux")
    bits = size.bit_length() - 1
    assert size == 1 << bits and bits >= 2
    count = pair_list.shape[0] // 3
    pair_list = pair_list.T
    half = virtuals // 2
    cube = 2 * virtuals * virtuals * width
    column = vir_energy[:, None]
    row = vir_energy[None, :]
    wide, narrow = (struct((count, half, virtuals), t) for t in (F32, BF16))

    sends = call(
        functools.partial(pick_body, count),
        [struct((count, virtuals, width), BF16)] * 2,
        [SM, pl.BlockSpec(memory_space=pltpu.HBM)],
        cube // 8,
        (pair_list, orbital_factors),
        [pltpu.SemaphoreType.DMA((2, count))],
    )
    arrived = [meet(sends[x], x) for x in PHASES]
    lists = [meet(pair_list, x) for x in PHASES]
    blocks = gathered(orbital_factors, bits)
    shape = (owned, virtuals, columns)
    wave = cube * owned
    low = [o for o in range(size) if o < 2]
    moved = call(
        functools.partial(moved_body, low, True),
        struct(shape, F32),
        [VM] * 3,
        2 * wave,
        (metric_factor, *[blocks[o] for o in low]),
    )
    for o in range(2, size - 1):
        moved = call(
            functools.partial(moved_body, [o], False),
            struct(shape, F32),
            [VM] * 3,
            wave,
            (metric_factor, moved, blocks[o]),
            alias={1: 0},
        )
    late, last = PHASES[-1], count - 1
    some = struct((count, virtuals, width), BF16)
    rest = struct((last, virtuals, width), BF16)
    lonely = lax.axis_size("orb") % 2 == 1
    keep0, send0, source0, early = call(
        functools.partial(integrals_body, 0),
        [wide, narrow, rest, struct((virtuals, width), BF16)],
        [SM] * 2 + [VM] * 2,
        count * cube,
        (pair_list, lists[0], orbital_factors, arrived[0]),
    )
    *denominators, seconds, number, alone_first = call(
        facts_body,
        [wide, wide, some, struct((8, 128), F32)] + [some] * lonely,
        [SM] * 4 + [VM] * 3,
        cube // 8,
        (pair_list, *lists, occ_energy, column, row, orbital_factors),
    ) + [None] * (not lonely)
    direct = count - 1
    moved, picked, chosen = call(
        functools.partial(moved_last_body, size - 1),
        [struct(shape, BF16), struct((virtuals, columns), BF16), struct((count, virtuals, columns), BF16)],
        [VM] * 4,
        wave,
        (metric_factor, moved, blocks[size - 1], number),
    )
    traded = meet(picked, PHASES[-1])

    source1 = arrived[1] + alone_first if lonely else arrived[1]
    keep1, send1 = call(chosen_integrals_body, [wide, narrow], [VM] * 2, count * cube, (seconds, source1))
    early_blocks = gathered(early, bits)

    keep, send = keep0, send0
    for bit in range(bits - 1):
        keep, send = call(add_body, [wide, narrow], [VM] * 2, cube // 8, (keep, flip(send, bit)))
    amps = call(amplitudes_body, narrow, [VM] * 3, cube // 8, (denominators[0], keep, flip(send, bits - 1)))
    back0, whole0 = call(
        terms_body,
        [struct((count, virtuals, columns), BF16), struct((count, virtuals, virtuals), BF16)],
        [VM] * 3,
        count * cube,
        (chosen, amps, flip(amps, 0)),
    )
    density0 = call(density_body, rest, [VM] * 2, last * cube, (source0, whole0))
    came0 = meet(back0, 0)
    blocks0 = gathered(density0, bits)

    own_amps, chosen = call(
        functools.partial(own_amplitudes_body, late),
        [narrow, struct((count, virtuals, columns), BF16)],
        [SM] * 3 + [VM] * (3 + size),
        cube * count * size // 2,
        (pair_list, lists[late], occ_energy, column, row, moved, *blocks),
    )
    keep, send = keep1, send1
    for bit in range(bits - 2):
        keep, send = call(add_body, [wide, narrow], [VM] * 2, cube // 8, (keep, flip(send, bit)))
    piece = struct((half, virtuals), BF16)
    keep, *sends = call(add_apart_body, [wide] + [piece] * count, [VM] * 2, cube // 8, (keep, flip(send, bits - 2)))
    wholes, backs, cames = [], [], []
    for s in range(count):
        amps = call(
            functools.partial(pair_amplitudes_body, s),
            piece,
            [VM] * 3,
            cube // 16,
            (denominators[1], keep, flip(sends[s], bits - 1)),
        )
        back, whole = call(
            functools.partial(pair_terms_body, s),
            [struct((virtuals, columns), BF16), struct((virtuals, virtuals), BF16)],
            [VM] * 3,
            cube,
            (chosen, amps, flip(amps, 0)),
        )
        wholes.append(whole)
        backs.append(back)
        cames.append(meet(back, late))
    density1 = call(pair_density_body, rest, [VM] * count, last * cube, (source1, *wholes[:last]))
    blocks1 = gathered(density1, bits)

    held = call(
        own_terms_body,
        struct(shape, F32),
        [SM] + [VM] * 3,
        2 * count * cube,
        (pair_list, moved, own_amps, flip(own_amps, 0)),
        [pltpu.VMEM((count, virtuals, virtuals), BF16)],
    )
    held = call(
        functools.partial(last_pairs_body, (0, last), (late, direct)),
        struct(shape, F32),
        [SM] * 3 + [VM] * (6 + size),
        cube,
        (pair_list, *lists, held, moved, whole0, wholes[last], traded, metric_factor, *early_blocks),
        alias={3: 0},
    )
    held = call(
        functools.partial(result0_body, [(0, range(size), True), (1, low, False)]),
        struct(shape, F32),
        [SM] * 3 + [VM] * (4 + size + len(low)),
        (size + 2) * last * cube,
        (pair_list, *lists, held, metric_factor, *blocks0, back0, came0, *[blocks1[o] for o in low]),
        alias={3: 0},
    )
    high = range(2, size)
    code, held = call(
        functools.partial(result1_body, [(1, high, False)], count),
        [struct((8, 128), F32), struct(shape, F32)],
        [SM] * 2 + [VM] * (1 + len(high) + 2 * count),
        last * len(high) * cube,
        (pair_list, lists[1], held, metric_factor, *[blocks1[o] for o in high], *backs, *cames[:last]),
        alias={2: 1},
    )
    return call(
        last_body,
        [struct(shape, BF16), struct(shape, F32)],
        [VM] * 3,
        cube // 8,
        (held, code, cames[last]),
        [pltpu.VMEM(shape, BF16), pltpu.SemaphoreType.DMA((owned,))],
        alias={0: 1},
        out_specs=[pl.BlockSpec(memory_space=pltpu.HBM), VM],
    )[0]


def solution(mesh):
    placed = (P("orb", None, "aux"), P(None, "aux"), P(), P(), P("orb", None))
    return jax.shard_map(local, mesh=mesh, in_specs=placed, out_specs=P("orb", None, "aux"), check_vma=False)
```
